32 devices in a mesh: row: 8 (over z, core), col: 4 (over y, x).
Axes of the slice: x: 2, y: 2, z: 4, core: 2. Of those that a mesh axis runs over, the one named last changes fastest.
Arguments:
- tile_left: bfloat16 [8, 4, 2048, 128], P('row', 'col'), may hold values from -6 to 6
- tile_right: bfloat16 [8, 4, 2048, 128], P('row', 'col'), may hold values from -1 to 1
- tile_blocks: int32 [8, 4], P('row', 'col'), may hold values from 1 to 4
- panel_left: bfloat16 [2, 8, 2048, 128], P(None, 'row', 'col'), may hold values from -6 to 6
- panel_right: bfloat16 [2, 8, 2048, 128], P(None, 'row', 'col'), may hold values from -2 to 2
- swap_flag: int32 [8, 4], P('row', 'col'), may hold values from 0 to 1, as said below
Outputs:
- grown_left: bfloat16 [8, 4, 2048, 256], P('row', 'col')
- grown_right: bfloat16 [8, 4, 2048, 256], P('row', 'col')
The draws below stay inside these ranges and needn't reach their ends.
Inputs may be any that keep to these rules, and one draw needn't show every extreme that they name: swap_flag[i, c] equals swap_flag[i, (c + 4 / 2) mod 4], so tiles change owner in pairs.
All inputs are finite; a program needn't handle non-finite values.
Results may differ from the reference program's by a relative error of at most 0.0057.
Values may be sent and summed in bfloat16 or wider, within the bound.
A program may use at most 64 MiB of HBM per device.

```python
import jax
import jax.numpy as jnp
from jax import lax

NB = 2048
RT = 128
RP = 128
RBLK = 32
N_ROW = 8
N_COL = 4


def draw_swap_flag(key, part):
    halves = jax.random.randint(jax.random.fold_in(key, 7), (N_ROW, N_COL // 2), 0, 2)
    return jnp.concatenate([halves, halves], axis=1).astype(jnp.int32)


def draw_panel_right(key, part):
    spread = 0.4 ** 0.5 * (RP * NB) ** (-0.25)
    shape = (2, N_ROW, NB, RP)
    noise = jnp.clip(jax.random.normal(jax.random.fold_in(key, 13), shape, jnp.float32), -6.0, 6.0) * spread
    stride = NB // RP
    rows = lax_rows = jnp.arange(NB, dtype=jnp.int32)
    cols = jnp.arange(RP, dtype=jnp.int32)
    ident = (rows[:, None] == cols[None, :] * stride).astype(jnp.float32)
    return (noise + ident[None, None]).astype(jnp.bfloat16)


def set_ends(array, key, low, largest):
    extent = array.shape
    index_at = [jax.random.randint(jax.random.fold_in(key, axis), (), 0, extent[axis]) for axis in range(len(extent))]
    array = array.at[tuple(index_at)].set(low)
    longest = extent.index(max(extent))
    index_at[longest] = (index_at[longest] + 1) % extent[longest]
    return array.at[tuple(index_at)].set(largest)


def level_of(rng, shape, pieces, low, top_value):
    loudness, own = 1.0, jax.random.fold_in(rng, 6)
    for position, parts in pieces:
        draws = jnp.exp(jax.random.uniform(jax.random.fold_in(own, position), (parts,), jnp.float32, low / len(pieces), top_value / len(pieces)))
        loudness = loudness * jnp.repeat(draws, shape[position] // parts).reshape([-1 if axis == position else 1 for axis in range(len(shape))])
    return loudness


def bell_draw(key, dims, scale, reach, cuts=(), held_as=jnp.bfloat16):
    entries = jax.random.normal(key, dims, jnp.float32) * scale
    if len(cuts) > 0:
        entries = level_of(key, dims, cuts, -0.22, 0.18) * entries
    return jnp.clip(entries, min=-reach, max=reach).astype(held_as)


def setup_inputs(seed: int = 0) -> dict:
    seeds = jax.random.split(jax.random.key(seed), 7)
    return {
        "tile_left": bell_draw(seeds[0], (N_ROW, N_COL, NB, RT), 1.0, 6.0, ((0, 8), (1, 4))),
        "tile_right": bell_draw(seeds[1], (N_ROW, N_COL, NB, RT), ((2 * RT) ** -0.5), 1.0, ((0, 8), (1, 4))),
        "tile_blocks": set_ends(jax.random.randint(seeds[2], (N_ROW, N_COL), 1, RT // RBLK + 1), jax.random.fold_in(seeds[2], 1), 1, (RT // RBLK + 1) - 1).astype(jnp.int32),
        "panel_left": bell_draw(seeds[3], (2, N_ROW, NB, RP), 1.0, 6.0, ((1, 8), (2, 4))),
        "panel_right": draw_panel_right(jax.random.fold_in(seeds[6], 71), 0),
        "swap_flag": draw_swap_flag(jax.random.fold_in(seeds[6], 71), 0),
    }


def expand(row_left, masked_left, masked_right, col_left, coupling, live_cols):
    lifted = (-jnp.dot(row_left.astype(jnp.float32), coupling.astype(jnp.float32), preferred_element_type=jnp.float32)).astype(jnp.bfloat16)
    stacked_left = jnp.concatenate([masked_left, lifted], axis=1)
    stacked_right = jnp.concatenate([masked_right, col_left], axis=1)
    dead_cols = jnp.concatenate([1.0 - live_cols.astype(jnp.float32), jnp.zeros((coupling.shape[1],), jnp.float32)])
    gram_matrix = jnp.dot(stacked_left.T.astype(jnp.float32), stacked_left.astype(jnp.float32), preferred_element_type=jnp.float32) / stacked_left.shape[0]
    gram_matrix = gram_matrix + jnp.diag(dead_cols)
    factor = jnp.linalg.cholesky(gram_matrix)
    left_out = lax.linalg.triangular_solve(factor, stacked_left.astype(jnp.float32), left_side=False, lower=True, transpose_a=True)
    right_out = jnp.dot(stacked_right.astype(jnp.float32), factor, precision=lax.Precision.HIGHEST)
    return (left_out.astype(jnp.bfloat16), right_out.astype(jnp.bfloat16))

def reference(tile_left, tile_right, tile_blocks, panel_left, panel_right, swap_flag):

    def one_tile(flat_index):
        row_index = flat_index // N_COL
        col_index = flat_index % N_COL
        live_mask = jnp.arange(RT, dtype=jnp.int32) < tile_blocks[row_index, col_index] * RBLK
        zero_value = jnp.zeros((), jnp.bfloat16)
        masked_left = jnp.where(live_mask[None, :], tile_left[row_index, col_index], zero_value)
        masked_right = jnp.where(live_mask[None, :], tile_right[row_index, col_index], zero_value)
        coupling = jnp.dot(panel_right[1, row_index].T.astype(jnp.float32), panel_right[0, col_index].astype(jnp.float32), preferred_element_type=jnp.float32).astype(jnp.bfloat16)
        return expand(panel_left[1, row_index], masked_left, masked_right, panel_left[0, col_index], coupling, live_mask.astype(jnp.float32))
    left_all, right_all = lax.map(one_tile, jnp.arange(N_ROW * N_COL, dtype=jnp.int32))
    left_all = left_all.reshape(N_ROW, N_COL, NB, RT + RP)
    right_all = right_all.reshape(N_ROW, N_COL, NB, RT + RP)
    chosen = (swap_flag == 1)[:, :, None, None]
    grown_left = jnp.where(chosen, jnp.roll(left_all, N_COL // 2, axis=1), left_all)
    grown_right = jnp.where(chosen, jnp.roll(right_all, N_COL // 2, axis=1), right_all)
    return (grown_left, grown_right)
```

```python
import functools

import jax
import jax.numpy as jnp
from jax import lax
from jax.experimental import pallas as pl
from jax.experimental.pallas import tpu as pltpu
from jax.sharding import PartitionSpec as P

RBLK = 32
MESH = pl.DeviceIdType.MESH
BF16 = jnp.bfloat16
F32 = jnp.float32


def exchange(R, C, u, v, pleft, pright, meta, uo, vo, rowo, colo, coupo, metao,
             ubuf, vbuf, rowbuf, colbuf, prbuf, psend, precv, mbuf,
             s_swap, r_swap, s_row, r_row, s_col, r_col, s_st, s_pr, r_pr, s_part, r_part, s_meta, r_meta, s_loc):
    r, c = lax.axis_index("row"), lax.axis_index("col")
    half = C // 2
    mate = lax.rem(c + half, C)
    sib = r + 1 - 2 * lax.rem(r, 2)
    has_up, has_dn = r + 2 < R, r >= 2

    def rcopy(src, dst, ss, rs, to):
        return pltpu.make_async_remote_copy(
            src_ref=src, dst_ref=dst, send_sem=ss, recv_sem=rs, device_id=to, device_id_type=MESH
        )

    barrier = pltpu.get_barrier_semaphore()
    for d in range(C):
        @pl.when(d != c)
        def _():
            pl.semaphore_signal(barrier, inc=1, device_id=(r, d), device_id_type=MESH)
    pl.semaphore_signal(barrier, inc=1, device_id=(sib, c), device_id_type=MESH)

    @pl.when(has_up)
    def _():
        pl.semaphore_signal(barrier, inc=1, device_id=(r + 2, c), device_id_type=MESH)

    @pl.when(has_dn)
    def _():
        pl.semaphore_signal(barrier, inc=1, device_id=(r - 2, c), device_id_type=MESH)

    peers = C + jnp.where(has_up, 1, 0) + jnp.where(has_dn, 1, 0)
    pl.semaphore_wait(barrier, peers)

    ends = []

    def send(cond, copy):
        @pl.when(cond)
        def _():
            copy.start()
        ends.append((cond, copy))

    loc_pr = pltpu.make_async_copy(pright.at[0], prbuf.at[lax.min(r, C - 1)], s_loc.at[0])
    is_src_pr = r < C

    def relay_sends(s, src, slot, ss, rs):
        par = lax.rem(r, 2) == lax.rem(s, 2)
        send(par & (r >= s) & has_up, rcopy(src, slot, ss.at[0], rs, (r + 2, c)))
        send(par & (r <= s) & has_dn, rcopy(src, slot, ss.at[1], rs, (r - 2, c)))
        send(par, rcopy(src, slot, ss.at[2], rs, (sib, c)))

    for d in range(C):
        send(c != d, rcopy(meta, mbuf.at[c], s_meta.at[d], r_meta.at[c], (r, d)))

    for s in range(C):
        slot, rs, ss = prbuf.at[s], r_pr.at[s], s_pr.at[s]
        send((r == s) & has_up, rcopy(pright.at[0], slot, ss.at[0], rs, (r + 2, c)))
        send((r == s) & has_dn, rcopy(pright.at[0], slot, ss.at[1], rs, (r - 2, c)))
        send(r == s, rcopy(pright.at[0], slot, ss.at[2], rs, (sib, c)))

    @pl.when(is_src_pr)
    def _():
        loc_pr.start()

    for t in range(2):
        d = lax.rem(r + t * half, C)
        send((r < C) & (d != c), rcopy(pleft.at[0], colbuf.at[t, c], s_st.at[t], r_col.at[t, c], (r, d)))
    tiles = (c, mate)
    loc_pl = []
    for t in range(2):
        copy = pltpu.make_async_copy(pleft.at[0], colbuf.at[t, c], s_loc.at[1 + t])
        loc_pl.append(copy)

        @pl.when(r == tiles[t])
        def _():
            copy.start()

    for d in range(C):
        send(c != d, rcopy(pleft.at[1], rowbuf.at[c], s_row.at[d], r_row.at[c], (r, d)))

    swap_u = rcopy(u, ubuf, s_swap.at[0], r_swap.at[0], (r, mate))
    swap_v = rcopy(v, vbuf, s_swap.at[1], r_swap.at[1], (r, mate))
    swap_u.start()
    swap_v.start()

    for s in range(C):
        slot, rs, ss = prbuf.at[s], r_pr.at[s], s_pr.at[s]

        @pl.when(r != s)
        def _():
            rcopy(slot, slot, ss.at[0], rs, (sib, c)).wait_recv()

        par = lax.rem(r, 2) == s % 2
        send(par & (r > s) & has_up, rcopy(slot, slot, ss.at[0], rs, (r + 2, c)))
        send(par & (r < s) & has_dn, rcopy(slot, slot, ss.at[1], rs, (r - 2, c)))
        send(par & (r != s), rcopy(slot, slot, ss.at[2], rs, (sib, c)))

    @pl.when(is_src_pr)
    def _():
        loc_pr.wait()

    for d in range(C):
        @pl.when(c != d)
        def _():
            rcopy(meta, mbuf.at[d], s_meta.at[d], r_meta.at[d], (r, d)).wait_recv()

        @pl.when(c == d)
        def _():
            mbuf[d] = meta[...]

    part = [
        lax.dot_general(pright[1], prbuf[s], (((0,), (0,)), ((), ())), preferred_element_type=F32)
        for s in range(C)
    ]
    for d in range(C):
        chosen = mbuf[d][0:1, :] > 0.5
        value = jnp.where(chosen, part[(d + half) % C], part[d])
        psend[d] = value

        @pl.when(c == d)
        def _():
            precv[d] = value
    for d in range(C):
        send(c != d, rcopy(psend.at[d], precv.at[c], s_part.at[d], r_part.at[c], (r, d)))

    for b in range(C):
        for t in range(2):
            slot, rs, ss = colbuf.at[t, b], r_col.at[t, b], s_col.at[t, b]
            mine = (r == tiles[t]) & (c == b)

            @pl.when(mine)
            def _():
                loc_pl[t].wait()

            @pl.when(jnp.logical_not(mine))
            def _():
                rcopy(slot, slot, ss.at[0], rs, (sib, c)).wait_recv()

            relay_sends(tiles[t], slot, slot, ss, rs)

    own_meta = meta[...]
    flagged = own_meta[0:1, :] > 0.5

    for d in range(C):
        @pl.when(c != d)
        def _():
            rcopy(pleft.at[1], rowbuf.at[d], s_row.at[d], r_row.at[d], (r, d)).wait_recv()
            rowo[d] = rowbuf[d]

        @pl.when(c == d)
        def _():
            rowo[d] = pleft[1]

    for b in range(C):
        colo[b] = jnp.where(flagged, colbuf[1, b], colbuf[0, b])

    swap_u.wait_recv()
    uo[...] = jnp.where(flagged, ubuf[...], u[...])
    swap_v.wait_recv()
    vo[...] = jnp.where(flagged, vbuf[...], v[...])
    for d in range(C):
        @pl.when(c != d)
        def _():
            rcopy(psend.at[d], precv.at[d], s_part.at[d], r_part.at[d], (r, d)).wait_recv()
    total = precv[0]
    for d in range(1, C):
        total = total + precv[d]
    coupo[...] = total.astype(BF16)
    metao[...] = jnp.where(flagged, mbuf[mate], own_meta)

    swap_u.wait_send()
    swap_v.wait_send()
    for cond, copy in ends:
        @pl.when(cond)
        def _():
            copy.wait_send()


def split3(x):
    h = x.astype(BF16)
    rest = x - h.astype(F32)
    m = rest.astype(BF16)
    return h, m, (rest - m.astype(F32)).astype(BF16)


def factor_rows(work, n, sb):
    lanes = 128
    sub = lax.broadcasted_iota(jnp.int32, (8, lanes), 0)
    groups = sb // 8

    def sub_row(x, k):
        return jnp.broadcast_to(x[k : k + 1, :], x.shape)

    for r0 in range(0, n, sb):
        a0 = r0 // lanes * lanes
        width = n + lanes
        tiles = width // lanes
        rows = [
            [work[r0 + 8 * g : r0 + 8 * g + 8, a0 + lanes * w : a0 + lanes * (w + 1)] for w in range(tiles)]
            for g in range(groups)
        ]
        for t in range(groups):
            base = r0 - a0 + 8 * t
            cols = [
                {g: jnp.broadcast_to(rows[g][0][:, base + i : base + i + 1], (8, lanes)) for g in range(t, groups)}
                for i in range(8)
            ]
            for k in range(8):
                inv = lax.rsqrt(sub_row(cols[k][t], k))
                scaled = {g: cols[k][g] * inv for g in range(t, groups)}
                for j in range(k + 1, 8):
                    lj = sub_row(scaled[t], j)
                    for g in range(t, groups):
                        cols[j][g] = cols[j][g] - scaled[g] * lj
                below = jnp.where(sub > k, scaled[t], 0.0)
                for w in range(tiles):
                    rowk = sub_row(rows[t][w], k) * inv
                    rows[t][w] = jnp.where(sub == k, rowk, rows[t][w] - below * rowk)
                    for g in range(t + 1, groups):
                        rows[g][w] = rows[g][w] - scaled[g] * rowk
        done = jnp.concatenate([jnp.concatenate(rows[g], axis=1) for g in range(groups)], axis=0)
        work[r0 : r0 + sb, a0 : a0 + width] = done
        r1 = r0 + sb
        if r1 < n:
            b0 = r1 // lanes * lanes
            h, m, l = split3(done)
            left = jnp.concatenate([h, h, m, m, h, l], axis=0)[:, b0 - a0 : n - a0]
            right = jnp.concatenate([h, m, h, m, l, h], axis=0)
            update = lax.dot_general(left, right, (((0,), (0,)), ((), ())), preferred_element_type=F32)
            work[r1:n, a0 : a0 + width] = work[r1:n, a0 : a0 + width] - update[r1 - b0 :, :]


def compute(chunk, u, v, row, col, coup, meta, lo, ro, stack, work):
    nb, rk = u.shape
    rp = coup.shape[1]
    n = rk + rp
    lane = lax.broadcasted_iota(jnp.int32, (1, rk), 1).astype(F32)
    live = lane < meta[1:2, :] * RBLK

    def fill(step, acc):
        at = pl.ds(pl.multiple_of(step * chunk, chunk), chunk)
        lifted = -jnp.dot(row[at, :], coup[...], preferred_element_type=F32)
        piece = jnp.concatenate(
            [jnp.where(live, u[at, :], jnp.zeros((), BF16)), lifted.astype(BF16)], axis=1
        )
        stack[at, :] = piece
        return acc + lax.dot_general(piece, piece, (((0,), (0,)), ((), ())), preferred_element_type=F32)

    gram = lax.fori_loop(0, nb // chunk, fill, jnp.zeros((n, n), F32)) / nb
    ri = lax.broadcasted_iota(jnp.int32, (n, n), 0)
    ci = lax.broadcasted_iota(jnp.int32, (n, n), 1)
    dead = jnp.concatenate([jnp.where(live, 0.0, 1.0).astype(F32), jnp.zeros((1, rp), F32)], axis=1)
    work[:, :n] = gram + jnp.where(ri == ci, dead, 0.0)
    work[:, n:] = jnp.where(ri == ci, 1.0, 0.0).astype(F32)
    factor_rows(work, n, 32)
    upper = jnp.where(ri <= ci, work[:, :n], 0.0)
    inverse = work[:, n:]
    uh, um, _ = split3(upper)
    ih, im, _ = split3(inverse)
    nt = (((1,), (1,)), ((), ()))

    def emit(step, _):
        at = pl.ds(pl.multiple_of(step * chunk, chunk), chunk)
        x = stack[at, :]
        left = lax.dot_general(x, ih, nt, preferred_element_type=F32)
        left = left + lax.dot_general(x, im, nt, preferred_element_type=F32)
        lo[at, :] = left.astype(BF16)
        y = jnp.concatenate([jnp.where(live, v[at, :], jnp.zeros((), BF16)), col[at, :]], axis=1)
        right = lax.dot_general(y, uh, nt, preferred_element_type=F32)
        right = right + lax.dot_general(y, um, nt, preferred_element_type=F32)
        ro[at, :] = right.astype(BF16)
        return 0

    lax.fori_loop(0, nb // chunk, emit, 0)


def per_device(R, C, tile_left, tile_right, tile_blocks, panel_left, panel_right, swap_flag):
    nb, rk = tile_left.shape[2:]
    blk, rp = panel_left.shape[2:]
    top = lax.broadcasted_iota(jnp.int32, (8, 128), 0) == 0
    meta = jnp.where(top, swap_flag[0, 0], tile_blocks[0, 0]).astype(F32)
    vm = pl.BlockSpec(memory_space=pltpu.VMEM)
    dma = pltpu.SemaphoreType.DMA
    S = jax.ShapeDtypeStruct
    uo, vo, rowo, colo, coup, metao = pl.pallas_call(
        functools.partial(exchange, R, C),
        out_shape=(
            S((nb, rk), BF16), S((nb, rk), BF16), S((C, blk, rp), BF16), S((C, blk, rp), BF16),
            S((rp, rp), BF16), S((8, 128), F32),
        ),
        in_specs=[vm] * 5,
        out_specs=[vm] * 6,
        scratch_shapes=[
            pltpu.VMEM((nb, rk), BF16), pltpu.VMEM((nb, rk), BF16),
            pltpu.VMEM((C, blk, rp), BF16), pltpu.VMEM((2, C, blk, rp), BF16), pltpu.VMEM((C, blk, rp), BF16),
            pltpu.VMEM((C, rp, rp), F32), pltpu.VMEM((C, rp, rp), F32), pltpu.VMEM((C, 8, 128), F32),
            dma((2,)), dma((2,)), dma((C,)), dma((C,)), dma((2, C, 3)), dma((2, C)), dma((2,)),
            dma((C, 3)), dma((C,)), dma((C,)), dma((C,)), dma((C,)), dma((C,)), dma((3,)),
        ],
        compiler_params=pltpu.CompilerParams(
            collective_id=0, has_side_effects=True, vmem_limit_bytes=40 * 1024 * 1024
        ),
        name="exchange",
    )(tile_left[0, 0], tile_right[0, 0], panel_left[:, 0], panel_right[:, 0], meta)
    n = rk + rp
    lo, ro = pl.pallas_call(
        functools.partial(compute, min(512, nb)),
        out_shape=(S((nb, n), BF16), S((nb, n), BF16)),
        in_specs=[vm] * 6,
        out_specs=[vm] * 2,
        scratch_shapes=[pltpu.VMEM((nb, n), BF16), pltpu.VMEM((n, 2 * n), F32)],
        compiler_params=pltpu.CompilerParams(vmem_limit_bytes=40 * 1024 * 1024),
        name="compute",
    )(uo, vo, rowo.reshape(nb, rp), colo.reshape(nb, rp), coup, metao)
    return lo[None, None], ro[None, None]


def solution(mesh):
    placed = (
        P("row", "col", None, None),
        P("row", "col", None, None),
        P("row", "col"),
        P(None, "row", "col", None),
        P(None, "row", "col", None),
        P("row", "col"),
    )
    return jax.shard_map(
        functools.partial(per_device, mesh.shape["row"], mesh.shape["col"]),
        mesh=mesh,
        in_specs=placed,
        out_specs=(P("row", "col", None, None), P("row", "col", None, None)),
        check_vma=False,
    )
```

```python
import functools

import jax
import jax.numpy as jnp
from jax import lax
from jax.experimental import pallas as pl
from jax.experimental.pallas import tpu as pltpu
from jax.sharding import PartitionSpec as P

RBLK = 32
MESH = pl.DeviceIdType.MESH
BF16 = jnp.bfloat16
F32 = jnp.float32


def exchange(R, C, u, v, pleft, pright, meta, stack, pair, uph, upm, inh, inm,
             ubuf, vbuf, uown, vown, pr1, rowbuf, colbuf, prbuf, psend, precv, mbuf, work,
             s_swap, r_swap, s_row, r_row, s_fwd, s_col, r_col, s_st, s_pr, r_pr, s_part, r_part, s_meta, r_meta,
             s_loc):
    r, c = lax.axis_index("row"), lax.axis_index("col")
    half = C // 2
    mate = lax.rem(c + half, C)
    sib = r + 1 - 2 * lax.rem(r, 2)
    has_up, has_dn = r + 2 < R, r >= 2
    nb, rk = u.shape
    blk, rp = pleft.shape[1:]
    n = rk + rp

    def rcopy(src, dst, ss, rs, to):
        return pltpu.make_async_remote_copy(
            src_ref=src, dst_ref=dst, send_sem=ss, recv_sem=rs, device_id=to, device_id_type=MESH
        )

    load_u = pltpu.make_async_copy(u, uown, s_loc.at[3])
    load_v = pltpu.make_async_copy(v, vown, s_loc.at[4])
    load_r = pltpu.make_async_copy(pright.at[1], pr1, s_loc.at[5])
    load_l = pltpu.make_async_copy(pleft.at[1], rowbuf.at[c], s_loc.at[6])
    load_r.start()
    load_l.start()
    load_u.start()
    load_v.start()

    barrier = pltpu.get_barrier_semaphore()
    for d in range(C):
        @pl.when(d != c)
        def _():
            pl.semaphore_signal(barrier, inc=1, device_id=(r, d), device_id_type=MESH)
    pl.semaphore_signal(barrier, inc=1, device_id=(sib, c), device_id_type=MESH)

    @pl.when(has_up)
    def _():
        pl.semaphore_signal(barrier, inc=1, device_id=(r + 2, c), device_id_type=MESH)

    @pl.when(has_dn)
    def _():
        pl.semaphore_signal(barrier, inc=1, device_id=(r - 2, c), device_id_type=MESH)

    peers = C + jnp.where(has_up, 1, 0) + jnp.where(has_dn, 1, 0)
    pl.semaphore_wait(barrier, peers)

    ends = []

    def send(cond, copy):
        @pl.when(cond)
        def _():
            copy.start()
        ends.append((cond, copy))

    loc_pr = pltpu.make_async_copy(pright.at[0], prbuf.at[lax.min(r, C - 1)], s_loc.at[0])
    is_src_pr = r < C

    def relay_sends(s, src, slot, ss, rs):
        par = lax.rem(r, 2) == lax.rem(s, 2)
        send(par & (r >= s) & has_up, rcopy(src, slot, ss.at[0], rs, (r + 2, c)))
        send(par & (r <= s) & has_dn, rcopy(src, slot, ss.at[1], rs, (r - 2, c)))
        send(par, rcopy(src, slot, ss.at[2], rs, (sib, c)))

    for d in range(C):
        send(c != d, rcopy(meta, mbuf.at[c], s_meta.at[d], r_meta.at[c], (r, d)))

    for s in range(C):
        slot, rs, ss = prbuf.at[s], r_pr.at[s], s_pr.at[s]
        send((r == s) & has_up, rcopy(pright.at[0], slot, ss.at[0], rs, (r + 2, c)))
        send((r == s) & has_dn, rcopy(pright.at[0], slot, ss.at[1], rs, (r - 2, c)))
        send(r == s, rcopy(pright.at[0], slot, ss.at[2], rs, (sib, c)))

    @pl.when(is_src_pr)
    def _():
        loc_pr.start()

    for t in range(2):
        d = lax.rem(r + t * half, C)
        send((r < C) & (d != c), rcopy(pleft.at[0], colbuf.at[t, c], s_st.at[t], r_col.at[t, c], (r, d)))
    tiles = (c, mate)
    loc_pl = []
    for t in range(2):
        copy = pltpu.make_async_copy(pleft.at[0], colbuf.at[t, c], s_loc.at[1 + t])
        loc_pl.append(copy)

        @pl.when(r == tiles[t])
        def _():
            copy.start()

    for d in range(C):
        same = (c // half) == d // half
        send((c != d) & (same | (mate == d)),
             rcopy(pleft.at[1], rowbuf.at[c], s_row.at[d], r_row.at[c], (r, d)))
    swap_u = rcopy(u, ubuf, s_swap.at[0], r_swap.at[0], (r, mate))
    swap_v = rcopy(v, vbuf, s_swap.at[1], r_swap.at[1], (r, mate))
    swap_u.start()

    rcopy(pleft.at[1], rowbuf.at[mate], s_row.at[0], r_row.at[mate], (r, mate)).wait_recv()
    for d in range(C):
        same = (c // half) == d // half
        send((c != d) & same, rcopy(rowbuf.at[mate], rowbuf.at[mate], s_fwd.at[d], r_row.at[mate], (r, d)))

    for s in range(C):
        slot, rs, ss = prbuf.at[s], r_pr.at[s], s_pr.at[s]

        @pl.when(r != s)
        def _():
            rcopy(slot, slot, ss.at[0], rs, (sib, c)).wait_recv()

        par = lax.rem(r, 2) == s % 2
        send(par & (r > s) & has_up, rcopy(slot, slot, ss.at[0], rs, (r + 2, c)))
        send(par & (r < s) & has_dn, rcopy(slot, slot, ss.at[1], rs, (r - 2, c)))
        send(par & (r != s), rcopy(slot, slot, ss.at[2], rs, (sib, c)))

    @pl.when(is_src_pr)
    def _():
        loc_pr.wait()

    for d in range(C):
        @pl.when(c != d)
        def _():
            rcopy(meta, mbuf.at[d], s_meta.at[d], r_meta.at[d], (r, d)).wait_recv()

        @pl.when(c == d)
        def _():
            mbuf[d] = meta[...]

    load_r.wait()
    part = [
        lax.dot_general(pr1[...], prbuf[s], (((0,), (0,)), ((), ())), preferred_element_type=F32)
        for s in range(C)
    ]
    for d in range(C):
        chosen = mbuf[d][0:1, :] > 0.5
        value = jnp.where(chosen, part[(d + half) % C], part[d])
        psend[d] = value

        @pl.when(c == d)
        def _():
            precv[d] = value
    for d in range(C):
        send(c != d, rcopy(psend.at[d], precv.at[c], s_part.at[d], r_part.at[c], (r, d)))

    swap_v.start()

    for b in range(C):
        for t in range(2):
            slot, rs, ss = colbuf.at[t, b], r_col.at[t, b], s_col.at[t, b]
            mine = (r == tiles[t]) & (c == b)

            @pl.when(mine)
            def _():
                loc_pl[t].wait()

            @pl.when(jnp.logical_not(mine))
            def _():
                rcopy(slot, slot, ss.at[0], rs, (sib, c)).wait_recv()

            relay_sends(tiles[t], slot, slot, ss, rs)

    own_meta = meta[...]
    flagged = own_meta[0:1, :] > 0.5
    chosen_meta = jnp.where(flagged, mbuf[mate], own_meta)
    lane = lax.broadcasted_iota(jnp.int32, (1, rk), 1).astype(F32)
    live = lane < chosen_meta[1:2, :] * RBLK
    zero = jnp.zeros((), BF16)

    load_l.wait()
    for d in range(C):
        @pl.when((c != d) & (mate != d))
        def _():
            rcopy(pleft.at[1], rowbuf.at[d], s_row.at[d], r_row.at[d], (r, d)).wait_recv()
    load_u.wait()
    swap_u.wait_recv()
    for d in range(C):
        @pl.when(c != d)
        def _():
            rcopy(psend.at[d], precv.at[d], s_part.at[d], r_part.at[d], (r, d)).wait_recv()
    total = precv[0]
    for d in range(1, C):
        total = total + precv[d]
    coup = total.astype(BF16)

    def fill(step, acc):
        at = pl.ds(pl.multiple_of(step * blk, blk), blk)
        lifted = -jnp.dot(rowbuf[step], coup, preferred_element_type=F32)
        left = jnp.where(flagged, ubuf[at, :], uown[at, :])
        piece = jnp.concatenate([jnp.where(live, left, zero), lifted.astype(BF16)], axis=1)
        stack[at, :] = piece
        return acc + lax.dot_general(piece, piece, (((0,), (0,)), ((), ())), preferred_element_type=F32)

    gram = lax.fori_loop(0, C, fill, jnp.zeros((n, n), F32)) / nb
    ri = lax.broadcasted_iota(jnp.int32, (n, n), 0)
    ci = lax.broadcasted_iota(jnp.int32, (n, n), 1)
    dead = jnp.concatenate([jnp.where(live, 0.0, 1.0).astype(F32), jnp.zeros((1, rp), F32)], axis=1)
    work[:, :n] = gram + jnp.where(ri == ci, dead, 0.0)
    work[:, n:] = jnp.where(ri == ci, 1.0, 0.0).astype(F32)
    factor_rows(work, n, 32)
    upper = jnp.where(ri <= ci, work[:, :n], 0.0)
    inverse = work[:, n:]
    uph[...], upm[...], _ = split3(upper)
    inh[...], inm[...], _ = split3(inverse)

    load_v.wait()
    swap_v.wait_recv()

    def fill_right(step, _):
        at = pl.ds(pl.multiple_of(step * blk, blk), blk)
        right = jnp.where(flagged, vbuf[at, :], vown[at, :])
        own = jnp.where(flagged, colbuf[1, step], colbuf[0, step])
        pair[at, :] = jnp.concatenate([jnp.where(live, right, zero), own], axis=1)
        return 0

    lax.fori_loop(0, C, fill_right, 0)

    swap_u.wait_send()
    swap_v.wait_send()
    for cond, copy in ends:
        @pl.when(cond)
        def _():
            copy.wait_send()


def split3(x):
    h = x.astype(BF16)
    rest = x - h.astype(F32)
    m = rest.astype(BF16)
    return h, m, (rest - m.astype(F32)).astype(BF16)


def factor_rows(work, n, sb):
    lanes = 128
    sub = lax.broadcasted_iota(jnp.int32, (8, lanes), 0)
    groups = sb // 8

    def sub_row(x, k):
        return jnp.broadcast_to(x[k : k + 1, :], x.shape)

    for r0 in range(0, n, sb):
        a0 = r0 // lanes * lanes
        width = n + lanes
        tiles = width // lanes
        rows = [
            [work[r0 + 8 * g : r0 + 8 * g + 8, a0 + lanes * w : a0 + lanes * (w + 1)] for w in range(tiles)]
            for g in range(groups)
        ]
        for t in range(groups):
            base = r0 - a0 + 8 * t
            cols = [
                {g: jnp.broadcast_to(rows[g][0][:, base + i : base + i + 1], (8, lanes)) for g in range(t, groups)}
                for i in range(8)
            ]
            for k in range(8):
                inv = lax.rsqrt(sub_row(cols[k][t], k))
                scaled = {g: cols[k][g] * inv for g in range(t, groups)}
                for j in range(k + 1, 8):
                    lj = sub_row(scaled[t], j)
                    for g in range(t, groups):
                        cols[j][g] = cols[j][g] - scaled[g] * lj
                below = jnp.where(sub > k, scaled[t], 0.0)
                for w in range(tiles):
                    rowk = sub_row(rows[t][w], k) * inv
                    rows[t][w] = jnp.where(sub == k, rowk, rows[t][w] - below * rowk)
                    for g in range(t + 1, groups):
                        rows[g][w] = rows[g][w] - scaled[g] * rowk
        done = jnp.concatenate([jnp.concatenate(rows[g], axis=1) for g in range(groups)], axis=0)
        work[r0 : r0 + sb, a0 : a0 + width] = done
        r1 = r0 + sb
        if r1 < n:
            b0 = r1 // lanes * lanes
            h, m, l = split3(done)
            left = jnp.concatenate([h, h, m, m, h, l], axis=0)[:, b0 - a0 : n - a0]
            right = jnp.concatenate([h, m, h, m, l, h], axis=0)
            update = lax.dot_general(left, right, (((0,), (0,)), ((), ())), preferred_element_type=F32)
            work[r1:n, a0 : a0 + width] = work[r1:n, a0 : a0 + width] - update[r1 - b0 :, :]


def products(x, y, uph, upm, inh, inm, lo, ro):
    nt = (((1,), (1,)), ((), ()))
    chunk = lo.shape[0]
    at = pl.ds(pl.multiple_of(pl.program_id(0) * chunk, chunk), chunk)

    def product(value, high, low):
        out = lax.dot_general(value, high[...], nt, preferred_element_type=F32)
        return (out + lax.dot_general(value, low[...], nt, preferred_element_type=F32)).astype(BF16)

    lo[...] = product(x[at, :], inh, inm)
    ro[...] = product(y[at, :], uph, upm)


def per_device(R, C, tile_left, tile_right, tile_blocks, panel_left, panel_right, swap_flag):
    nb, rk = tile_left.shape[2:]
    blk, rp = panel_left.shape[2:]
    n = rk + rp
    top = lax.broadcasted_iota(jnp.int32, (8, 128), 0) == 0
    meta = jnp.where(top, swap_flag[0, 0], tile_blocks[0, 0]).astype(F32)
    vm = pl.BlockSpec(memory_space=pltpu.VMEM)
    hbm = pl.BlockSpec(memory_space=pltpu.HBM)
    dma = pltpu.SemaphoreType.DMA
    S = jax.ShapeDtypeStruct
    V = pltpu.VMEM
    parts = pl.pallas_call(
        functools.partial(exchange, R, C),
        out_shape=(S((nb, n), BF16),) * 2 + (S((n, n), BF16),) * 4,
        in_specs=[hbm] * 4 + [vm],
        out_specs=[vm] * 6,
        scratch_shapes=[
            V((nb, rk), BF16), V((nb, rk), BF16), V((nb, rk), BF16), V((nb, rk), BF16), V((blk, rp), BF16),
            V((C, blk, rp), BF16), V((2, C, blk, rp), BF16), V((C, blk, rp), BF16),
            V((C, rp, rp), F32), V((C, rp, rp), F32), V((C, 8, 128), F32), V((n, 2 * n), F32),
            dma((2,)), dma((2,)), dma((C,)), dma((C,)), dma((C,)), dma((2, C, 3)), dma((2, C)), dma((2,)),
            dma((C, 3)), dma((C,)), dma((C,)), dma((C,)), dma((C,)), dma((C,)), dma((7,)),
        ],
        compiler_params=pltpu.CompilerParams(
            collective_id=0, has_side_effects=True, vmem_limit_bytes=24 * 1024 * 1024
        ),
        name="exchange",
    )(tile_left[0, 0], tile_right[0, 0], panel_left[:, 0], panel_right[:, 0], meta)
    piece = pl.BlockSpec((min(512, nb), n), lambda i: (i, 0))
    lo, ro = pl.pallas_call(
        products,
        grid=(nb // min(512, nb),),
        out_shape=(S((nb, n), BF16),) * 2,
        in_specs=[vm] * 6,
        out_specs=[piece] * 2,
        compiler_params=pltpu.CompilerParams(vmem_limit_bytes=24 * 1024 * 1024),
        name="products",
    )(*parts)
    return lo[None, None], ro[None, None]


def solution(mesh):
    placed = (
        P("row", "col", None, None),
        P("row", "col", None, None),
        P("row", "col"),
        P(None, "row", "col", None),
        P(None, "row", "col", None),
        P("row", "col"),
    )
    return jax.shard_map(
        functools.partial(per_device, mesh.shape["row"], mesh.shape["col"]),
        mesh=mesh,
        in_specs=placed,
        out_specs=(P("row", "col", None, None), P("row", "col", None, None)),
        check_vma=False,
    )
```

```python
import functools

import jax
import jax.numpy as jnp
from jax import lax
from jax.experimental import pallas as pl
from jax.experimental.pallas import tpu as pltpu
from jax.sharding import PartitionSpec as P

RBLK = 32
MESH = pl.DeviceIdType.MESH
BF16 = jnp.bfloat16
F32 = jnp.float32


def exchange(R, C, u, v, pleft, pright, meta, stack, pair, uph, upm, inh, inm,
             ubuf, vbuf, uown, vown, pr1, rowbuf, colbuf, prbuf, psend, precv, mbuf, work,
             s_swap, r_swap, s_row, r_row, s_fwd, s_col, r_col, s_st, s_pr, r_pr, s_part, r_part, s_meta, r_meta,
             s_loc):
    r, c = lax.axis_index("row"), lax.axis_index("col")
    half = C // 2
    mate = lax.rem(c + half, C)
    sib = r + 1 - 2 * lax.rem(r, 2)
    has_up, has_dn = r + 2 < R, r >= 2
    nb, rk = u.shape
    blk, rp = pleft.shape[1:]
    n = rk + rp

    def rcopy(src, dst, ss, rs, to):
        return pltpu.make_async_remote_copy(
            src_ref=src, dst_ref=dst, send_sem=ss, recv_sem=rs, device_id=to, device_id_type=MESH
        )

    load_u = pltpu.make_async_copy(u, uown, s_loc.at[3])
    load_v = pltpu.make_async_copy(v, vown, s_loc.at[4])
    load_r = pltpu.make_async_copy(pright.at[1], pr1, s_loc.at[5])
    load_l = pltpu.make_async_copy(pleft.at[1], rowbuf.at[c], s_loc.at[6])
    load_r.start()
    load_l.start()
    load_u.start()
    load_v.start()

    barrier = pltpu.get_barrier_semaphore()
    for d in range(C):
        @pl.when(d != c)
        def _():
            pl.semaphore_signal(barrier, inc=1, device_id=(r, d), device_id_type=MESH)
    pl.semaphore_signal(barrier, inc=1, device_id=(sib, c), device_id_type=MESH)

    @pl.when(has_up)
    def _():
        pl.semaphore_signal(barrier, inc=1, device_id=(r + 2, c), device_id_type=MESH)

    @pl.when(has_dn)
    def _():
        pl.semaphore_signal(barrier, inc=1, device_id=(r - 2, c), device_id_type=MESH)

    peers = C + jnp.where(has_up, 1, 0) + jnp.where(has_dn, 1, 0)
    pl.semaphore_wait(barrier, peers)

    ends = []

    def send(cond, copy):
        @pl.when(cond)
        def _():
            copy.start()
        ends.append((cond, copy))

    loc_pr = pltpu.make_async_copy(pright.at[0], prbuf.at[lax.min(r, C - 1)], s_loc.at[0])
    is_src_pr = r < C

    def relay_sends(s, src, slot, ss, rs):
        par = lax.rem(r, 2) == lax.rem(s, 2)
        send(par & (r >= s) & has_up, rcopy(src, slot, ss.at[0], rs, (r + 2, c)))
        send(par & (r <= s) & has_dn, rcopy(src, slot, ss.at[1], rs, (r - 2, c)))
        send(par, rcopy(src, slot, ss.at[2], rs, (sib, c)))

    for d in range(C):
        send(c != d, rcopy(meta, mbuf.at[c], s_meta.at[d], r_meta.at[c], (r, d)))

    for s in range(C):
        slot, rs, ss = prbuf.at[s], r_pr.at[s], s_pr.at[s]
        send((r == s) & has_up, rcopy(pright.at[0], slot, ss.at[0], rs, (r + 2, c)))
        send((r == s) & has_dn, rcopy(pright.at[0], slot, ss.at[1], rs, (r - 2, c)))
        send(r == s, rcopy(pright.at[0], slot, ss.at[2], rs, (sib, c)))

    @pl.when(is_src_pr)
    def _():
        loc_pr.start()

    for t in range(2):
        d = lax.rem(r + t * half, C)
        send((r < C) & (d != c), rcopy(pleft.at[0], colbuf.at[t, c], s_st.at[t], r_col.at[t, c], (r, d)))
    tiles = (c, mate)
    loc_pl = []
    for t in range(2):
        copy = pltpu.make_async_copy(pleft.at[0], colbuf.at[t, c], s_loc.at[1 + t])
        loc_pl.append(copy)

        @pl.when(r == tiles[t])
        def _():
            copy.start()

    for d in range(C):
        same = (c // half) == d // half
        send((c != d) & (same | (mate == d)),
             rcopy(pleft.at[1], rowbuf.at[c], s_row.at[d], r_row.at[c], (r, d)))
    swap_u = rcopy(u, ubuf, s_swap.at[0], r_swap.at[0], (r, mate))
    swap_v = rcopy(v, vbuf, s_swap.at[1], r_swap.at[1], (r, mate))

    for s in range(C):
        slot, rs, ss = prbuf.at[s], r_pr.at[s], s_pr.at[s]

        @pl.when(r != s)
        def _():
            rcopy(slot, slot, ss.at[0], rs, (sib, c)).wait_recv()

        par = lax.rem(r, 2) == s % 2
        send(par & (r > s) & has_up, rcopy(slot, slot, ss.at[0], rs, (r + 2, c)))
        send(par & (r < s) & has_dn, rcopy(slot, slot, ss.at[1], rs, (r - 2, c)))
        send(par & (r != s), rcopy(slot, slot, ss.at[2], rs, (sib, c)))

    rcopy(pleft.at[1], rowbuf.at[mate], s_row.at[0], r_row.at[mate], (r, mate)).wait_recv()
    for d in range(C):
        same = (c // half) == d // half
        send((c != d) & same, rcopy(rowbuf.at[mate], rowbuf.at[mate], s_fwd.at[d], r_row.at[mate], (r, d)))

    swap_u.start()

    @pl.when(is_src_pr)
    def _():
        loc_pr.wait()

    for d in range(C):
        @pl.when(c != d)
        def _():
            rcopy(meta, mbuf.at[d], s_meta.at[d], r_meta.at[d], (r, d)).wait_recv()

        @pl.when(c == d)
        def _():
            mbuf[d] = meta[...]

    load_r.wait()
    part = [
        lax.dot_general(pr1[...], prbuf[s], (((0,), (0,)), ((), ())), preferred_element_type=F32)
        for s in range(C)
    ]
    for d in range(C):
        chosen = mbuf[d][0:1, :] > 0.5
        value = jnp.where(chosen, part[(d + half) % C], part[d])
        psend[d] = value

        @pl.when(c == d)
        def _():
            precv[d] = value
    for d in range(C):
        send(c != d, rcopy(psend.at[d], precv.at[c], s_part.at[d], r_part.at[c], (r, d)))

    swap_v.start()

    for b in range(C):
        for t in range(2):
            slot, rs, ss = colbuf.at[t, b], r_col.at[t, b], s_col.at[t, b]
            mine = (r == tiles[t]) & (c == b)

            @pl.when(mine)
            def _():
                loc_pl[t].wait()

            @pl.when(jnp.logical_not(mine))
            def _():
                rcopy(slot, slot, ss.at[0], rs, (sib, c)).wait_recv()

            relay_sends(tiles[t], slot, slot, ss, rs)

    own_meta = meta[...]
    flagged = own_meta[0:1, :] > 0.5
    chosen_meta = jnp.where(flagged, mbuf[mate], own_meta)
    lane = lax.broadcasted_iota(jnp.int32, (1, rk), 1).astype(F32)
    live = lane < chosen_meta[1:2, :] * RBLK
    zero = jnp.zeros((), BF16)

    load_l.wait()
    for d in range(C):
        @pl.when((c != d) & (mate != d))
        def _():
            rcopy(pleft.at[1], rowbuf.at[d], s_row.at[d], r_row.at[d], (r, d)).wait_recv()
    load_u.wait()
    swap_u.wait_recv()
    for d in range(C):
        @pl.when(c != d)
        def _():
            rcopy(psend.at[d], precv.at[d], s_part.at[d], r_part.at[d], (r, d)).wait_recv()
    total = precv[0]
    for d in range(1, C):
        total = total + precv[d]
    coup = total.astype(BF16)

    def fill(step, acc):
        at = pl.ds(pl.multiple_of(step * blk, blk), blk)
        lifted = -jnp.dot(rowbuf[step], coup, preferred_element_type=F32)
        left = jnp.where(flagged, ubuf[at, :], uown[at, :])
        piece = jnp.concatenate([jnp.where(live, left, zero), lifted.astype(BF16)], axis=1)
        stack[at, :] = piece
        return acc + lax.dot_general(piece, piece, (((0,), (0,)), ((), ())), preferred_element_type=F32)

    gram = lax.fori_loop(0, C, fill, jnp.zeros((n, n), F32)) / nb
    ri = lax.broadcasted_iota(jnp.int32, (n, n), 0)
    ci = lax.broadcasted_iota(jnp.int32, (n, n), 1)
    dead = jnp.concatenate([jnp.where(live, 0.0, 1.0).astype(F32), jnp.zeros((1, rp), F32)], axis=1)
    work[:, :n] = gram + jnp.where(ri == ci, dead, 0.0)
    work[:, n:] = jnp.where(ri == ci, 1.0, 0.0).astype(F32)
    factor_rows(work, n, 32)
    upper = jnp.where(ri <= ci, work[:, :n], 0.0)
    inverse = work[:, n:]
    uph[...], upm[...], _ = split3(upper)
    inh[...], inm[...], _ = split3(inverse)

    load_v.wait()
    swap_v.wait_recv()

    def fill_right(step, _):
        at = pl.ds(pl.multiple_of(step * blk, blk), blk)
        right = jnp.where(flagged, vbuf[at, :], vown[at, :])
        own = jnp.where(flagged, colbuf[1, step], colbuf[0, step])
        pair[at, :] = jnp.concatenate([jnp.where(live, right, zero), own], axis=1)
        return 0

    lax.fori_loop(0, C, fill_right, 0)

    swap_u.wait_send()
    swap_v.wait_send()
    for cond, copy in ends:
        @pl.when(cond)
        def _():
            copy.wait_send()


def split3(x):
    h = x.astype(BF16)
    rest = x - h.astype(F32)
    m = rest.astype(BF16)
    return h, m, (rest - m.astype(F32)).astype(BF16)


def factor_rows(work, n, sb):
    lanes = 128
    sub = lax.broadcasted_iota(jnp.int32, (8, lanes), 0)
    groups = sb // 8

    def sub_row(x, k):
        return jnp.broadcast_to(x[k : k + 1, :], x.shape)

    for r0 in range(0, n, sb):
        a0 = r0 // lanes * lanes
        width = n + lanes
        tiles = width // lanes
        rows = [
            [work[r0 + 8 * g : r0 + 8 * g + 8, a0 + lanes * w : a0 + lanes * (w + 1)] for w in range(tiles)]
            for g in range(groups)
        ]
        for t in range(groups):
            base = r0 - a0 + 8 * t
            cols = [
                {g: jnp.broadcast_to(rows[g][0][:, base + i : base + i + 1], (8, lanes)) for g in range(t, groups)}
                for i in range(8)
            ]
            for k in range(8):
                inv = lax.rsqrt(sub_row(cols[k][t], k))
                scaled = {g: cols[k][g] * inv for g in range(t, groups)}
                for j in range(k + 1, 8):
                    lj = sub_row(scaled[t], j)
                    for g in range(t, groups):
                        cols[j][g] = cols[j][g] - scaled[g] * lj
                below = jnp.where(sub > k, scaled[t], 0.0)
                for w in range(tiles):
                    rowk = sub_row(rows[t][w], k) * inv
                    rows[t][w] = jnp.where(sub == k, rowk, rows[t][w] - below * rowk)
                    for g in range(t + 1, groups):
                        rows[g][w] = rows[g][w] - scaled[g] * rowk
        done = jnp.concatenate([jnp.concatenate(rows[g], axis=1) for g in range(groups)], axis=0)
        work[r0 : r0 + sb, a0 : a0 + width] = done
        r1 = r0 + sb
        if r1 < n:
            b0 = r1 // lanes * lanes
            h, m, l = split3(done)
            left = jnp.concatenate([h, h, m, m, h, l], axis=0)[:, b0 - a0 : n - a0]
            right = jnp.concatenate([h, m, h, m, l, h], axis=0)
            update = lax.dot_general(left, right, (((0,), (0,)), ((), ())), preferred_element_type=F32)
            work[r1:n, a0 : a0 + width] = work[r1:n, a0 : a0 + width] - update[r1 - b0 :, :]


def products(x, y, uph, upm, inh, inm, lo, ro):
    nt = (((1,), (1,)), ((), ()))

    def product(value, high, low):
        out = lax.dot_general(value, high[...], nt, preferred_element_type=F32)
        return (out + lax.dot_general(value, low[...], nt, preferred_element_type=F32)).astype(BF16)

    lo[...] = product(x[...], inh, inm)
    ro[...] = product(y[...], uph, upm)


def per_device(R, C, tile_left, tile_right, tile_blocks, panel_left, panel_right, swap_flag):
    nb, rk = tile_left.shape[2:]
    blk, rp = panel_left.shape[2:]
    n = rk + rp
    top = lax.broadcasted_iota(jnp.int32, (8, 128), 0) == 0
    meta = jnp.where(top, swap_flag[0, 0], tile_blocks[0, 0]).astype(F32)
    vm = pl.BlockSpec(memory_space=pltpu.VMEM)
    hbm = pl.BlockSpec(memory_space=pltpu.HBM)
    dma = pltpu.SemaphoreType.DMA
    S = jax.ShapeDtypeStruct
    V = pltpu.VMEM
    parts = pl.pallas_call(
        functools.partial(exchange, R, C),
        out_shape=(S((nb, n), BF16),) * 2 + (S((n, n), BF16),) * 4,
        in_specs=[hbm] * 4 + [vm],
        out_specs=[vm] * 6,
        scratch_shapes=[
            V((nb, rk), BF16), V((nb, rk), BF16), V((nb, rk), BF16), V((nb, rk), BF16), V((blk, rp), BF16),
            V((C, blk, rp), BF16), V((2, C, blk, rp), BF16), V((C, blk, rp), BF16),
            V((C, rp, rp), F32), V((C, rp, rp), F32), V((C, 8, 128), F32), V((n, 2 * n), F32),
            dma((2,)), dma((2,)), dma((C,)), dma((C,)), dma((C,)), dma((2, C, 3)), dma((2, C)), dma((2,)),
            dma((C, 3)), dma((C,)), dma((C,)), dma((C,)), dma((C,)), dma((C,)), dma((7,)),
        ],
        compiler_params=pltpu.CompilerParams(
            collective_id=0, has_side_effects=True, vmem_limit_bytes=58 * 1024 * 1024
        ),
        name="exchange",
    )(tile_left[0, 0], tile_right[0, 0], panel_left[:, 0], panel_right[:, 0], meta)
    piece = pl.BlockSpec((min(512, nb), n), lambda i: (i, 0))
    lo, ro = pl.pallas_call(
        products,
        grid=(nb // min(512, nb),),
        out_shape=(S((nb, n), BF16),) * 2,
        in_specs=[piece] * 2 + [pl.BlockSpec((n, n), lambda i: (0, 0))] * 4,
        out_specs=[piece] * 2,
        name="products",
    )(*parts)
    return lo[None, None], ro[None, None]


def solution(mesh):
    placed = (
        P("row", "col", None, None),
        P("row", "col", None, None),
        P("row", "col"),
        P(None, "row", "col", None),
        P(None, "row", "col", None),
        P("row", "col"),
    )
    return jax.shard_map(
        functools.partial(per_device, mesh.shape["row"], mesh.shape["col"]),
        mesh=mesh,
        in_specs=placed,
        out_specs=(P("row", "col", None, None), P("row", "col", None, None)),
        check_vma=False,
    )
```
